32 devices in a mesh: dp: 8 (over z, core), mp: 4 (over y, x).
Axes of the slice: x: 2, y: 2, z: 4, core: 2. Of those that a mesh axis runs over, the one named last changes fastest.
Arguments:
- features: bfloat16 [8192, 8192], P('dp', 'mp'), may hold values from -6 to 6
- v_weight: bfloat16 [3, 8192, 1024], P(None, 'mp', 'dp'), may hold values from -0.0625 to 0.0625
- u_weight: bfloat16 [3, 1024, 8192], P(None, 'dp', 'mp'), may hold values from -0.1875 to 0.1875
- cross_bias: float32 [3, 8192], P(None, 'mp'), may hold values from -3 to 3
Outputs:
- crossed: bfloat16 [8192, 8192], P('dp', 'mp')
The draws below stay inside these ranges and needn't reach their ends.
All inputs are finite; a program needn't handle non-finite values.
Results may differ from the reference program's by a relative error of at most 0.009.
Values may be sent and summed in bfloat16 or wider, within the bound.
A program may use at most 128 MiB of HBM per device.

```python
import jax
import jax.numpy as jnp

D = 8192
R = 1024
LAYERS = 3
BATCH = 8192


def block_levels(key, extent, split, low, top_value):
    factor_of = 1.0
    for axis_at, blocks in split:
        draws = jax.random.uniform(jax.random.fold_in(jax.random.fold_in(key, 6), axis_at), (blocks,), jnp.float32, low / len(split), top_value / len(split))
        factor_of = factor_of * jnp.repeat(jnp.exp(draws), extent[axis_at] // blocks).reshape((-1,) + (1,) * (len(extent) - 1 - axis_at))
    return factor_of


def scatter_about(key, shape, width, reach, shards=(), kind=jnp.bfloat16):
    entries = jax.random.normal(key, shape, jnp.float32) * width
    if len(shards) > 0:
        entries = block_levels(key, shape, shards, -0.22, 0.18) * entries
    return jnp.clip(entries, min=-reach, max=reach).astype(kind)


def setup_inputs(seed: int = 0) -> dict:
    key_of = jax.random.split(jax.random.key(seed), 5)
    features = scatter_about(key_of[0], (BATCH, D), 1.0, 6.0, ((0, 8), (1, 4)))
    v_weight = scatter_about(key_of[1], (LAYERS, D, R), D ** -0.5, 0.0625, ((1, 4), (2, 8)))
    u_weight = scatter_about(key_of[2], (LAYERS, R, D), R ** -0.5, 0.1875, ((1, 8), (2, 4)))
    cross_bias = scatter_about(key_of[3], (LAYERS, D), 0.5, 3.0, ((1, 4),), jnp.float32)
    return {"features": features, "v_weight": v_weight, "u_weight": u_weight, "cross_bias": cross_bias}


def reference(features, v_weight, u_weight, cross_bias):
    carried = features
    for layer_number in range(LAYERS):
        rank_proj = jnp.dot(carried, v_weight[layer_number], preferred_element_type=jnp.float32).astype(jnp.bfloat16)
        cross_term = jnp.dot(rank_proj, u_weight[layer_number], preferred_element_type=jnp.float32) + cross_bias[layer_number]
        carried = (features.astype(jnp.float32) * cross_term + carried.astype(jnp.float32)).astype(jnp.bfloat16)
    return carried
```

```python
import functools

import jax
import jax.numpy as jnp
from jax import lax
from jax.experimental import pallas as pl
from jax.experimental.pallas import tpu as pltpu
from jax.sharding import PartitionSpec as P

MESH = pl.DeviceIdType.MESH
HOPS = (2, -2, 1, -1)


def kernel(nz, n, vt_ref, u_ref, f_ref, b_ref, out_ref, w, pf, sbuf, rbuf, rank,
           loc, zsend, zrecv, fsend, psend, precv, rs_s, rs_r, ag_s, ag_r):
    layers, rs, cols = vt_ref.shape
    rows = f_ref.shape[0]
    seg = rows // n
    ck = 2 * rs
    dp, me = lax.axis_index("dp"), lax.axis_index("mp")
    z, c = dp // 2, dp % 2
    step = jnp.where(2 * z < nz, 1, -1)

    def dev(zt, ct, m):
        return {"dp": zt * 2 + ct, "mp": m}

    def copy_to(src, dst, send, recv, device):
        return pltpu.make_async_remote_copy(
            src_ref=src, dst_ref=dst, send_sem=send, recv_sem=recv,
            device_id=device, device_id_type=MESH)

    def order(i):
        return lax.rem(z + step * i + nz, nz)

    def valid(d):
        return (z + d >= 0) & (z + d < nz)

    def blk(p, s, cc):
        return w.at[p, pl.ds(pl.multiple_of((s * 2 + cc) * rs, rs), rs)]

    def local_copy(p):
        src = (vt_ref if p % 2 == 0 else u_ref).at[p // 2]
        return pltpu.make_async_copy(src, blk(p, z, c), loc.at[p])

    def direct(p, k):
        return copy_to(blk(p, z, c), blk(p, z, c), zsend.at[p, k], zrecv.at[p, z],
                       dev(z + HOPS[k], c, me))

    def arrival(p, s):
        return copy_to(blk(p, s, c), blk(p, s, c), fsend.at[p, s], zrecv.at[p, s], dev(z, 1 - c, me))

    def relays(s):
        return ((s >= z + 2) & (z >= 1)) | ((s <= z - 2) & (z <= nz - 2))

    def relay(p, s):
        return copy_to(blk(p, s, c), blk(p, s, c), fsend.at[p, s], zrecv.at[p, s],
                       dev(jnp.where(s > z, z - 1, z + 1), c, me))

    def push(p, s):
        return copy_to(blk(p, s, c), blk(p, s, c), psend.at[p, s], precv.at[p, s], dev(z, 1 - c, me))

    def pushed(p, s):
        return copy_to(blk(p, s, 1 - c), blk(p, s, 1 - c), psend.at[p, s], precv.at[p, s],
                       dev(z, 1 - c, me))

    def issue_own(p):
        local_copy(p).wait()
        for k in range(len(HOPS)):
            @pl.when(valid(HOPS[k]))
            def _():
                direct(p, k).start()

    def take(p, s):
        @pl.when(s != z)
        def _():
            arrival(p, s).wait_recv()

        @pl.when(relays(s))
        def _():
            relay(p, s).start()

        push(p, s).start()

    def lanes(s):
        return pl.ds(pl.multiple_of(s * ck, ck), ck)

    def seg_rows(m):
        return pl.ds(pl.multiple_of(m * seg, seg), seg)

    def other(k):
        return lax.rem(me + k, n)

    for p in range(2 * layers):
        local_copy(p).start()
    barrier = pltpu.get_barrier_semaphore()
    for k in range(1, n):
        pl.semaphore_signal(barrier, inc=1, device_id=dev(z, c, other(k)), device_id_type=MESH)
    pl.semaphore_signal(barrier, inc=1, device_id=dev(z, 1 - c, me), device_id_type=MESH)
    for d in HOPS:
        @pl.when(valid(d))
        def _():
            pl.semaphore_signal(barrier, inc=1, device_id=dev(z + d, c, me), device_id_type=MESH)
    pl.semaphore_wait(barrier, n + jnp.minimum(z, 2) + jnp.minimum(nz - 1 - z, 2))

    issue_own(0)
    issue_own(1)

    for l in range(layers):
        pv, pu = 2 * l, 2 * l + 1
        cur = f_ref if l == 0 else out_ref

        def sum_out(s, k):
            t = other(k)
            return copy_to(sbuf.at[seg_rows(t), lanes(s)], rbuf.at[l, me, :, lanes(s)],
                           rs_s.at[s, k - 1], rs_r.at[s, me], dev(z, c, t))

        def sum_in(s, k):
            q = other(k)
            return copy_to(sbuf.at[seg_rows(q), lanes(s)], rbuf.at[l, q, :, lanes(s)],
                           rs_s.at[s, k - 1], rs_r.at[s, q], dev(z, c, q))

        def rank_out(s, k):
            mine = rank.at[l, seg_rows(me), lanes(s)]
            return copy_to(mine, mine, ag_s.at[s, k - 1], ag_r.at[s, me], dev(z, c, other(k)))

        def rank_in(s, k):
            q = other(k)
            theirs = rank.at[l, seg_rows(q), lanes(s)]
            return copy_to(theirs, theirs, ag_s.at[s, k - 1], ag_r.at[s, q], dev(z, c, q))

        def reduce(s):
            acc = pf[seg_rows(me), lanes(s)]
            for k in range(1, n):
                sum_in(s, k).wait_recv()
                acc = acc + rbuf[l, other(k), :, lanes(s)].astype(jnp.float32)
            rank[l, seg_rows(me), lanes(s)] = acc.astype(jnp.bfloat16)
            for k in range(1, n):
                rank_out(s, k).start()

        @pl.loop(0, nz)
        def _(i):
            s = order(i)
            take(pv, s)
            pushed(pv, s).wait_recv()
            part = lax.dot_general(cur[...], w[pv, lanes(s), :], (((1,), (1,)), ((), ())),
                                   preferred_element_type=jnp.float32)
            pf[:, lanes(s)] = part
            sbuf[:, lanes(s)] = part.astype(jnp.bfloat16)
            for k in range(1, n):
                sum_out(s, k).start()

            @pl.when(i > 0)
            def _():
                reduce(order(i - 1))

        if pv + 2 < 2 * layers:
            issue_own(pv + 2)
        reduce(order(nz - 1))

        @pl.loop(0, nz)
        def _(i):
            take(pu, order(i))

        if pu + 2 < 2 * layers:
            issue_own(pu + 2)

        @pl.loop(0, nz)
        def _(i):
            s = order(i)
            pushed(pu, s).wait_recv()
            for k in range(1, n):
                rank_in(s, k).wait_recv()

        cb = 256 if cols % 256 == 0 else cols

        @pl.loop(0, cols // cb)
        def _(j):
            at = pl.ds(pl.multiple_of(j * cb, cb), cb)
            cross = jnp.dot(rank[l], w[pu, :, at], preferred_element_type=jnp.float32)
            cross = cross + b_ref[l, at][None, :]
            out_ref[:, at] = (f_ref[:, at].astype(jnp.float32) * cross
                              + cur[:, at].astype(jnp.float32)).astype(jnp.bfloat16)

        @pl.loop(0, nz)
        def _(s):
            for k in range(1, n):
                sum_out(s, k).wait_send()
                rank_out(s, k).wait_send()

    for p in range(2 * layers):
        for k in range(len(HOPS)):
            @pl.when(valid(HOPS[k]))
            def _():
                direct(p, k).wait_send()

        @pl.loop(0, nz)
        def _(s):
            push(p, s).wait_send()

            @pl.when(relays(s))
            def _():
                relay(p, s).wait_send()


def solution(mesh):
    n = mesh.shape["mp"]
    nz = mesh.shape["dp"] // 2

    def local(features, v_weight, u_weight, cross_bias):
        layers, rs, cols = u_weight.shape
        rows = features.shape[0]
        r = rs * nz * 2
        pieces = 2 * layers
        vt = jnp.swapaxes(v_weight, 1, 2)
        vm = pl.BlockSpec(memory_space=pltpu.VMEM)
        hbm = pl.BlockSpec(memory_space=pl.ANY)
        dma = pltpu.SemaphoreType.DMA
        return pl.pallas_call(
            functools.partial(kernel, nz, n),
            out_shape=jax.ShapeDtypeStruct((rows, cols), jnp.bfloat16),
            in_specs=[hbm, hbm, vm, vm],
            out_specs=vm,
            scratch_shapes=[
                pltpu.VMEM((pieces, r, cols), jnp.bfloat16),
                pltpu.VMEM((rows, r), jnp.float32),
                pltpu.VMEM((rows, r), jnp.bfloat16),
                pltpu.VMEM((layers, n, rows // n, r), jnp.bfloat16),
                pltpu.VMEM((layers, rows, r), jnp.bfloat16),
                dma((pieces,)), dma((pieces, len(HOPS))), dma((pieces, nz)), dma((pieces, nz)),
                dma((pieces, nz)), dma((pieces, nz)),
                dma((nz, n)), dma((nz, n)), dma((nz, n)), dma((nz, n)),
            ],
            compiler_params=pltpu.CompilerParams(
                collective_id=0, has_side_effects=True, vmem_limit_bytes=67043328),
            name="cross_layers",
        )(vt, u_weight, features, cross_bias)

    return jax.shard_map(
        local,
        mesh=mesh,
        in_specs=(P("dp", "mp"), P(None, "mp", "dp"), P(None, "dp", "mp"), P(None, "mp")),
        out_specs=P("dp", "mp"),
        check_vma=False,
    )
```

```python
import functools

import jax
import jax.numpy as jnp
from jax import lax
from jax.experimental import pallas as pl
from jax.experimental.pallas import tpu as pltpu
from jax.sharding import PartitionSpec as P

MESH = pl.DeviceIdType.MESH
HOPS = (1, -1)


def kernel(nz, n, native, v_ref, u_ref, x_ref, b_ref, y_ref, wv, wu, f_ref, out_ref, pf, sbuf, rbuf,
           rank, loc, zsend, zrecv, fsend, psend, precv, rs_s, rs_r, ag_s, ag_r, in_s, out_s):
    layers, rs, cols = u_ref.shape
    rows = x_ref.shape[0]
    seg = rows // n
    ck = 2 * rs
    cb = 256 if cols % 256 == 0 else cols
    dp, me = lax.axis_index("dp"), lax.axis_index("mp")
    z, c = dp // 2, dp % 2
    step = jnp.where(2 * z < nz, 1, -1)

    def dev(zt, ct, m):
        return {"dp": zt * 2 + ct, "mp": m}

    def copy_to(src, dst, send, recv, device):
        return pltpu.make_async_remote_copy(
            src_ref=src, dst_ref=dst, send_sem=send, recv_sem=recv,
            device_id=device, device_id_type=MESH)

    def order(i):
        near = jnp.minimum(z, nz - 1 - z)
        zigzag = jnp.where(i % 2 == 1, -((i + 1) // 2), i // 2)
        return z + step * jnp.where(i <= 2 * near, zigzag, i - near)

    def valid(d):
        return (z + d >= 0) & (z + d < nz)

    def blk(p, s, cc):
        if native and p % 2 == 0:
            return wv.at[p // 2, s, :, pl.ds(pl.multiple_of(cc * rs, rs), rs)]
        w = wu if p % 2 else wv
        return w.at[p // 2, pl.ds(pl.multiple_of((s * 2 + cc) * rs, rs), rs)]

    def local_copy(p):
        src = (v_ref if p % 2 == 0 else u_ref).at[p // 2]
        return pltpu.make_async_copy(src, blk(p, z, c), loc.at[p])

    def direct(p, k):
        return copy_to(blk(p, z, c), blk(p, z, c), zsend.at[p, k], zrecv.at[p, z],
                       dev(z + HOPS[k], c, me))

    def arrival(p, s):
        return copy_to(blk(p, s, c), blk(p, s, c), fsend.at[p, s], zrecv.at[p, s], dev(z, 1 - c, me))

    def relays(s):
        return ((s > z) & (z >= 1)) | ((s < z) & (z <= nz - 2))

    def relay(p, s):
        return copy_to(blk(p, s, c), blk(p, s, c), fsend.at[p, s], zrecv.at[p, s],
                       dev(jnp.where(s > z, z - 1, z + 1), c, me))

    def push(p, s):
        return copy_to(blk(p, s, c), blk(p, s, c), psend.at[p, s], precv.at[p, s], dev(z, 1 - c, me))

    def pushed(p, s):
        return copy_to(blk(p, s, 1 - c), blk(p, s, 1 - c), psend.at[p, s], precv.at[p, s],
                       dev(z, 1 - c, me))

    def held(d):
        return (z >= 1) & (z <= nz - 2)

    def issue_own(p, first):
        for k in range(len(HOPS)):
            hold = held(HOPS[k])

            @pl.when(valid(HOPS[k]) & (jnp.logical_not(hold) if first else hold))
            def _():
                direct(p, k).start()

    def take(p, s):
        @pl.when(s != z)
        def _():
            arrival(p, s).wait_recv()

        @pl.when(relays(s))
        def _():
            relay(p, s).start()

        push(p, s).start()

    def lanes(s):
        return pl.ds(pl.multiple_of(s * ck, ck), ck)

    def seg_rows(m):
        return pl.ds(pl.multiple_of(m * seg, seg), seg)

    def other(k):
        return lax.rem(me + k, n)

    def block_out(j):
        at = pl.ds(pl.multiple_of(j * cb, cb), cb)
        return pltpu.make_async_copy(out_ref.at[:, at], y_ref.at[:, at], out_s.at[j])

    whole_in = pltpu.make_async_copy(x_ref, f_ref, in_s)
    for p in range(2 * layers):
        local_copy(p).start()
    whole_in.start()
    barrier = pltpu.get_barrier_semaphore()
    for k in range(1, n):
        pl.semaphore_signal(barrier, inc=1, device_id=dev(z, c, other(k)), device_id_type=MESH)
    pl.semaphore_signal(barrier, inc=1, device_id=dev(z, 1 - c, me), device_id_type=MESH)
    for d in HOPS:
        @pl.when(valid(d))
        def _():
            pl.semaphore_signal(barrier, inc=1, device_id=dev(z + d, c, me), device_id_type=MESH)
    pl.semaphore_wait(barrier, n + jnp.minimum(z, 1) + jnp.minimum(nz - 1 - z, 1))

    for p in range(2 * layers):
        local_copy(p).wait()
        issue_own(p, True)
        if p < 2:
            issue_own(p, False)
    whole_in.wait()

    for l in range(layers):
        pv, pu = 2 * l, 2 * l + 1
        cur = f_ref if l == 0 else out_ref

        def sum_out(s, k):
            t = other(k)
            return copy_to(sbuf.at[seg_rows(t), lanes(s)], rbuf.at[l, me, :, lanes(s)],
                           rs_s.at[s, k - 1], rs_r.at[s, me], dev(z, c, t))

        def sum_in(s, k):
            q = other(k)
            return copy_to(sbuf.at[seg_rows(q), lanes(s)], rbuf.at[l, q, :, lanes(s)],
                           rs_s.at[s, k - 1], rs_r.at[s, q], dev(z, c, q))

        def rank_out(s, k):
            mine = rank.at[l, seg_rows(me), lanes(s)]
            return copy_to(mine, mine, ag_s.at[s, k - 1], ag_r.at[s, me], dev(z, c, other(k)))

        def rank_in(s, k):
            q = other(k)
            theirs = rank.at[l, seg_rows(q), lanes(s)]
            return copy_to(theirs, theirs, ag_s.at[s, k - 1], ag_r.at[s, q], dev(z, c, q))

        def reduce(s):
            acc = pf[seg_rows(me), lanes(s)]
            for k in range(1, n):
                sum_in(s, k).wait_recv()
                acc = acc + rbuf[l, other(k), :, lanes(s)].astype(jnp.float32)
            rank[l, seg_rows(me), lanes(s)] = acc.astype(jnp.bfloat16)
            for k in range(1, n):
                rank_out(s, k).start()

        @pl.loop(0, nz)
        def _(i):
            s = order(i)
            take(pv, s)
            pushed(pv, s).wait_recv()
            if native:
                part = jnp.dot(cur[...], wv[l, s], preferred_element_type=jnp.float32)
            else:
                part = lax.dot_general(cur[...], wv[l, lanes(s), :], (((1,), (1,)), ((), ())),
                                       preferred_element_type=jnp.float32)
            pf[:, lanes(s)] = part
            sbuf[:, lanes(s)] = part.astype(jnp.bfloat16)
            for k in range(1, n):
                sum_out(s, k).start()

            @pl.when(i > 0)
            def _():
                reduce(order(i - 1))

        if pv + 2 < 2 * layers:
            issue_own(pv + 2, False)
        reduce(order(nz - 1))

        @pl.loop(0, nz)
        def _(i):
            take(pu, order(i))

        if pu + 2 < 2 * layers:
            issue_own(pu + 2, False)

        @pl.loop(0, nz)
        def _(i):
            s = order(i)
            pushed(pu, s).wait_recv()
            for k in range(1, n):
                rank_in(s, k).wait_recv()


        @pl.loop(0, cols // cb)
        def _(j):
            at = pl.ds(pl.multiple_of(j * cb, cb), cb)
            cross = jnp.dot(rank[l], wu[l, :, at], preferred_element_type=jnp.float32)
            cross = cross + b_ref[l, at][None, :]
            out_ref[:, at] = (f_ref[:, at].astype(jnp.float32) * cross
                              + cur[:, at].astype(jnp.float32)).astype(jnp.bfloat16)
            if l == layers - 1:
                @pl.when(j > 0)
                def _():
                    block_out(j - 1).start()

        if l == layers - 1:
            block_out(cols // cb - 1).start()

        @pl.loop(0, nz)
        def _(s):
            for k in range(1, n):
                sum_out(s, k).wait_send()
                rank_out(s, k).wait_send()

    for p in range(2 * layers):
        for k in range(len(HOPS)):
            @pl.when(valid(HOPS[k]))
            def _():
                direct(p, k).wait_send()

        @pl.loop(0, nz)
        def _(s):
            push(p, s).wait_send()

            @pl.when(relays(s))
            def _():
                relay(p, s).wait_send()

    @pl.loop(0, cols // cb)
    def _(j):
        block_out(j).wait()


def solution(mesh):
    n = mesh.shape["mp"]
    nz = mesh.shape["dp"] // 2

    def local(features, v_weight, u_weight, cross_bias):
        layers, rs, cols = u_weight.shape
        rows = features.shape[0]
        r = rs * nz * 2
        pieces = 2 * layers
        native = rs % 128 == 0
        v = v_weight if native else jnp.swapaxes(v_weight, 1, 2)
        vm = pl.BlockSpec(memory_space=pltpu.VMEM)
        hbm = pl.BlockSpec(memory_space=pl.ANY)
        dma = pltpu.SemaphoreType.DMA
        return pl.pallas_call(
            functools.partial(kernel, nz, n, native),
            out_shape=jax.ShapeDtypeStruct((rows, cols), jnp.bfloat16),
            in_specs=[hbm, hbm, hbm, vm],
            out_specs=hbm,
            scratch_shapes=[
                pltpu.VMEM((layers, nz, cols, 2 * rs) if native else (layers, r, cols), jnp.bfloat16),
                pltpu.VMEM((layers, r, cols), jnp.bfloat16),
                pltpu.VMEM((rows, cols), jnp.bfloat16),
                pltpu.VMEM((rows, cols), jnp.bfloat16),
                pltpu.VMEM((rows, r), jnp.float32),
                pltpu.VMEM((rows, r), jnp.bfloat16),
                pltpu.VMEM((layers, n, rows // n, r), jnp.bfloat16),
                pltpu.VMEM((layers, rows, r), jnp.bfloat16),
                dma((pieces,)), dma((pieces, len(HOPS))), dma((pieces, nz)), dma((pieces, nz)),
                dma((pieces, nz)), dma((pieces, nz)),
                dma((nz, n)), dma((nz, n)), dma((nz, n)), dma((nz, n)),
                dma, dma((cols // (256 if cols % 256 == 0 else cols),)),
            ],
            compiler_params=pltpu.CompilerParams(
                collective_id=0, has_side_effects=True, vmem_limit_bytes=67043328),
            name="cross_layers",
        )(v, u_weight, features, cross_bias)

    return jax.shard_map(
        local,
        mesh=mesh,
        in_specs=(P("dp", "mp"), P(None, "mp", "dp"), P(None, "dp", "mp"), P(None, "mp")),
        out_specs=P("dp", "mp"),
        check_vma=False,
    )
```
